256 devices in a mesh: group: 2 (over z), seq: 128 (over y, x, core).
Axes of the slice: x: 8, y: 8, z: 2, core: 2. Of those that a mesh axis runs over, the one named last changes fastest.
The devices are a block of a 8x8x16 slice.
Arguments:
- tokens: bfloat16 [131072, 4096], P(('group', 'seq')), parts along dimension 0, may hold values from -6 to 6
- norm_gain: bfloat16 [4096], replicated, may hold values from 0.099609375 to 1.8984375
- w_key: bfloat16 [4096, 1024], P('seq'), may hold values from -0.09375 to 0.09375
- w_value: bfloat16 [4096, 1024], P('seq'), may hold values from -0.09375 to 0.09375
- lengths: int32 [4], P('group'), parts along dimension 0, may hold values from 16384 to 32768
- page_table: int32 [8192], P(('group', 'seq')), parts along dimension 0, may hold values from 0 to 5119, as said below
Outputs:
- kv_cache: bfloat16 [2, 10240, 16, 1024], P(None, ('group', 'seq')), parts along dimension 1
The draws below stay inside these ranges and needn't reach their ends.
There are 2 independent parts, one for each index of `group`. The reference program is written for one: setup_inputs(seed, part) draws one part's arguments, and reference() takes and returns one part's arrays. A program takes and returns all parts, laid end to end along the dimension named above; an argument that names none is the same for every part. Nothing has to cross between parts.
Inputs may be any that keep to these rules, and one draw needn't show every extreme that they name: The entries are distinct. Page g of the 32 pages of device s goes to slot page_table[g] of decode device page_table[g] // 40, which is s + k modulo 128 for an offset k in -2 .. 2, at a slot of the block of 8 slots from (k + 2) * 8 on; so at most 8 pages go from one device to one decode device, and exactly 8 from every device to some decode device.
All inputs are finite; a program needn't handle non-finite values.
Results may differ from the reference program's by a relative error of at most 0.0049.
Values may be sent and summed in bfloat16 or wider, within the bound.
A program may use at most 64 MiB of HBM per device.

```python
import jax
import jax.numpy as jnp
from jax import lax

D = 4096
HEAD = 128
PAGE = 16
REACH = 2
TOK_DEV = 512
KVD = 1024
TOKENS = 65536
LENGTH = 32768
CAP = 8
SLOTS = 40
PAGES = 4096
N_SEQ = 128


def draw_page_table(key, part):
    pages_dev = TOK_DEV // PAGE
    regions = 2 * REACH + 1

    def one_device(device):
        device_key = jax.random.fold_in(jax.random.fold_in(key, 7), device)
        first_key, second_key, third_key = jax.random.split(device_key, 3)
        full_region = jax.random.randint(first_key, (), 0, regions)
        ranks = jax.random.permutation(second_key, SLOTS)
        region_of = jnp.arange(SLOTS, dtype=jnp.int32) // CAP
        score = jnp.where(region_of == full_region, 0, SLOTS) + ranks
        order = jnp.argsort(score, stable=True)
        chosen = jax.random.permutation(third_key, order[:pages_dev])
        offset = chosen // CAP - REACH
        target = (device + offset) % N_SEQ
        return (target * SLOTS + chosen).astype(jnp.int32)
    table = jax.vmap(one_device)(jnp.arange(N_SEQ, dtype=jnp.int32))
    return table.reshape(-1).astype(jnp.int32)


def block_levels(key, shape, shards, low, top_value):
    factor_of = 1.0
    for axis_at, parts in shards:
        heights = jax.random.uniform(jax.random.fold_in(jax.random.fold_in(key, 6), axis_at), (parts,), jnp.float32, low / len(shards), top_value / len(shards))
        factor_of = factor_of * jnp.repeat(jnp.exp(heights), shape[axis_at] // parts).reshape((-1,) + (1,) * (len(shape) - 1 - axis_at))
    return factor_of


def bell_draw(own_key, extent, spread, most, cuts=(), kind=jnp.bfloat16):
    values = jax.random.normal(own_key, extent, jnp.float32) * spread
    if len(cuts) > 0:
        values = block_levels(own_key, extent, cuts, -0.22, 0.18) * values
    return jnp.clip(values, min=-most, max=most).astype(kind)


def setup_inputs(seed: int = 0, part: int = 0) -> dict:
    key_list = jax.random.split(jax.random.key(seed), 7)
    part_splits = jax.random.split(jax.random.fold_in(key_list[6], part), 7)
    return {
        "tokens": bell_draw(part_splits[0], (TOKENS, D), 1.0, 6.0, ((0, 128),)),
        "norm_gain": jnp.clip(1.0 + 0.18 * jax.random.normal(key_list[1], (D,), jnp.float32), 0.099609375, 1.8984375).astype(jnp.bfloat16),
        "w_key": bell_draw(key_list[2], (D, KVD), D ** -0.5, 0.09375, ((0, 128),)),
        "w_value": bell_draw(key_list[3], (D, KVD), D ** -0.5, 0.09375, ((0, 128),)),
        "lengths": jax.random.randint(part_splits[4], (2,), LENGTH // 2, LENGTH + 1).astype(jnp.int32),
        "page_table": draw_page_table(jax.random.fold_in(jax.random.fold_in(key_list[6], part), 71), part),
    }


ROPE_THETA = 500000.0
EPS = 1e-05

def rotate_keys(key_rows, position):
    half = HEAD // 2
    freq = ROPE_THETA ** (-(jnp.arange(half, dtype=jnp.float32) * 2.0 / HEAD))
    angle = position.astype(jnp.float32)[:, None] * freq[None, :]
    cosine = jnp.cos(angle)[:, None, :]
    sine = jnp.sin(angle)[:, None, :]
    shaped = key_rows.reshape(key_rows.shape[0], -1, HEAD)
    first = shaped[:, :, :half]
    second = shaped[:, :, half:]
    turned = jnp.concatenate([first * cosine - second * sine, second * cosine + first * sine], axis=2)
    return turned.reshape(key_rows.shape)

def reference(tokens, norm_gain, w_key, w_value, lengths, page_table):
    wide = tokens.astype(jnp.float32)
    scale = lax.rsqrt(lax.optimization_barrier(jnp.mean(wide * wide, axis=1, keepdims=True)) + EPS)
    normed = (wide * scale * norm_gain.astype(jnp.float32)[None, :]).astype(jnp.bfloat16)
    key_rows = jnp.dot(normed, w_key, preferred_element_type=jnp.float32)
    value_rows = jnp.dot(normed, w_value, preferred_element_type=jnp.float32)
    token_index = jnp.arange(TOKENS, dtype=jnp.int32)
    prompt_id = token_index // LENGTH
    position = token_index % LENGTH
    limit = jnp.where(prompt_id == 0, lengths[0], lengths[1])
    inside = (position < limit)[:, None]
    key_rows = rotate_keys(key_rows, position)
    keys = jnp.where(inside, key_rows, 0.0).astype(jnp.bfloat16)
    values = jnp.where(inside, value_rows, 0.0).astype(jnp.bfloat16)
    pages = jnp.stack([keys, values]).reshape(2, PAGES, PAGE, KVD)
    cache = jnp.zeros((2, N_SEQ * SLOTS, PAGE, KVD), jnp.bfloat16)
    return cache.at[:, page_table.astype(jnp.int32)].set(pages)
```

```python
import functools
import math

import jax
import jax.numpy as jnp
import numpy as np
from jax import lax
from jax.experimental import pallas as pl
from jax.experimental.pallas import tpu as pltpu
from jax.sharding import PartitionSpec as P

HEAD = 128
PAGE = 16
REACH = 2
CAP = 8
SLOTS = 40
PROMPTS = 2

ROPE_THETA = 500000.0
EPS = 1e-05

MESH = pl.DeviceIdType.MESH
CHUNKS = 4
FIRST = 32
SECOND = 16


def kernel(
    side,
    tokens_hbm,
    gain_ref,
    freq_ref,
    wk_hbm,
    wv_hbm,
    lengths_ref,
    table_ref,
    table_hbm,
    out,
    rows,
    weights,
    stage,
    total,
    cosine,
    sine,
    parcel,
    table_vec,
    table_smem,
    slot_vec,
    slot_smem,
    local_sem,
    swap_send,
    swap_recv,
    xs_send,
    xs_recv,
    ys_send,
    ys_recv,
    xb_send,
    xb_recv,
    yb_send,
    yb_recv,
    z_send,
    z_recv,
    page_send,
    page_recv,
):
    n_tok, depth = tokens_hbm.shape
    width = weights.shape[4]
    half_cols = width * (CHUNKS // 2)
    reach = side // 2
    half = side // 2
    block = weights.shape[3]

    group = lax.axis_index("group")
    me = lax.axis_index("seq")
    core = me % 2
    chip = me // 2
    x = chip % side
    y = chip // side
    chips = side * side
    parity = group % 2

    def device(yy, xx, cc):
        index = (((yy + side) % side) * side + (xx + side) % side) * 2 + cc
        return (group, index)

    partner = (group, chip * 2 + 1 - core)
    opposite = (group + 1 - 2 * parity, me)
    next_chip = (chip + 1) % chips
    prev_chip = (chip + chips - 1) % chips
    x_to = {1: device(y, x + 1, core), -1: device(y, x - 1, core)}
    y_to = {1: device(y + 1, x, core), -1: device(y - 1, x, core)}

    first_rows = pl.ds(0, FIRST)
    second_rows = pl.ds(pl.multiple_of(FIRST + SECOND * parity, SECOND), SECOND)
    other_rows = pl.ds(pl.multiple_of(FIRST + SECOND * (1 - parity), SECOND), SECOND)
    shard_second = pl.ds(pl.multiple_of(SECOND * parity, SECOND), SECOND)

    sent = []

    def remote(src, dst, send_sem, recv_sem, to):
        return pltpu.make_async_remote_copy(
            src_ref=src,
            dst_ref=dst,
            send_sem=send_sem,
            recv_sem=recv_sem,
            device_id=to,
            device_id_type=MESH,
        )

    token_parts = 4
    part = n_tok // token_parts

    def token_local(i):
        return pltpu.make_async_copy(
            tokens_hbm.at[pl.ds(i * part, part)],
            rows.at[pl.ds(pl.multiple_of(core * n_tok + i * part, part), part)],
            local_sem.at[i],
        )

    def token_swap(i):
        return remote(
            tokens_hbm.at[pl.ds(i * part, part)],
            rows.at[pl.ds(pl.multiple_of(core * n_tok + i * part, part), part)],
            swap_send.at[i],
            swap_recv.at[i],
            partner,
        )

    def token_arrival(i):
        there = rows.at[pl.ds(pl.multiple_of((1 - core) * n_tok + i * part, part), part)]
        return remote(there, there, swap_send.at[i], swap_recv.at[i], partner)

    def columns_of(q, cc):
        return pl.ds(pl.multiple_of(cc * half_cols + (q % 2) * width, 128), width)

    def shard(q):
        return wk_hbm if q < CHUNKS // 2 else wv_hbm

    def own_first(q):
        return pltpu.make_async_copy(
            shard(q).at[:, columns_of(q, core)],
            weights.at[q, y, x, first_rows, :],
            local_sem.at[token_parts + q],
        )

    def own_second(q):
        return pltpu.make_async_copy(
            shard(q).at[shard_second, columns_of(q, core)],
            weights.at[q, y, x, second_rows, :],
            local_sem.at[token_parts + q],
        )

    def staged(kv):
        source = (wk_hbm, wv_hbm)[kv]
        return pltpu.make_async_copy(
            source.at[:, pl.ds(pl.multiple_of((1 - core) * half_cols, 128), half_cols)],
            stage.at[kv],
            local_sem.at[token_parts + CHUNKS + kv],
        )

    def give_first(q):
        return remote(
            stage.at[q // 2, :, pl.ds((q % 2) * width, width)],
            weights.at[q, y, x, first_rows, :],
            swap_send.at[token_parts + q],
            swap_recv.at[token_parts + q],
            partner,
        )

    def give_second(q):
        return remote(
            stage.at[q // 2, shard_second, pl.ds((q % 2) * width, width)],
            weights.at[q, y, x, second_rows, :],
            swap_send.at[token_parts + q],
            swap_recv.at[token_parts + q],
            partner,
        )

    def give_table():
        i = token_parts + CHUNKS
        return remote(
            table_hbm, table_vec, swap_send.at[i], swap_recv.at[i], partner
        )

    for kv in range(2):
        staged(kv).start()

    @pl.when(core == 0)
    def _():
        for q in range(CHUNKS):
            own_first(q).start()

    @pl.when(core == 1)
    def _():
        for q in range(CHUNKS):
            own_second(q).start()

    for i in range(token_parts):
        token_local(i).start()

    barrier = pltpu.get_barrier_semaphore()
    friends = [x_to[1], x_to[-1], y_to[1], y_to[-1], partner, opposite]
    for other in (next_chip, prev_chip):
        for cc in range(2):
            friends.append((group, other * 2 + cc))
    for friend in friends:
        pl.semaphore_signal(barrier, inc=1, device_id=friend, device_id_type=MESH)
    pl.semaphore_wait(barrier, len(friends))

    for kv in range(2):
        staged(kv).wait()

    @pl.when(core == 0)
    def _():
        for q in range(CHUNKS):
            give_first(q).start()

    @pl.when(core == 1)
    def _():
        for q in range(CHUNKS):
            give_second(q).start()

    give_table().start()
    for i in range(token_parts):
        token_swap(i).start()

    parts = ((0, 1), (1, CHUNKS - 1))

    def x_short(g, s, d, origin, to):
        q0, nq = parts[g]
        piece = weights.at[pl.ds(q0, nq), y, (origin + 2 * side) % side, first_rows, :]
        return remote(piece, piece, xs_send.at[g, (1 - d) // 2, s - 1], xs_recv.at[g, (1 - d) // 2, s - 1], to)

    def y_short(g, s, d, origin, to):
        q0, nq = parts[g]
        piece = weights.at[pl.ds(q0, nq), (origin + 2 * side) % side, x, second_rows, :]
        return remote(piece, piece, ys_send.at[g, (1 - d) // 2, s - 1], ys_recv.at[g, (1 - d) // 2, s - 1], to)

    def short_runs(g, s, d):
        return s < reach or d == (1 if g == 0 else -1)

    def short_send(g, s):
        for d in (1, -1):
            if short_runs(g, s, d):
                x_short(g, s, d, x - d * (s - 1), x_to[d]).start()
                y_short(g, s, d, y - d * (s - 1), y_to[d]).start()

    def short_wait(g, s):
        for d in (1, -1):
            if short_runs(g, s, d):
                x_short(g, s, d, x - d * s, x_to[d]).wait_recv()
                y_short(g, s, d, y - d * s, y_to[d]).wait_recv()

    def short_done(g, s):
        for d in (1, -1):
            if short_runs(g, s, d):
                x_short(g, s, d, x - d * (s - 1), x_to[d]).wait_send()
                y_short(g, s, d, y - d * (s - 1), y_to[d]).wait_send()

    def block_ready(g):
        q0, nq = parts[g]

        @pl.when(core == 0)
        def _():
            for q in range(q0, q0 + nq):
                own_first(q).wait()
                give_second(q).wait_recv()

        @pl.when(core == 1)
        def _():
            for q in range(q0, q0 + nq):
                own_second(q).wait()
                give_first(q).wait_recv()

    def half_at(h):
        return pl.ds(h * half, half)

    def long_halves(s, d):
        if s < reach:
            return (0, 1)
        return (0,) if d == 1 else (1,)

    def long_index(s, h):
        return 2 * (s - 1) + (h if s < reach else 0)

    def y_long(q, s, h, d, origin, to):
        piece = weights.at[q, (origin + 2 * side) % side, half_at(h), first_rows, :]
        i = long_index(s, h)
        return remote(piece, piece, yb_send.at[q, (1 - d) // 2, i], yb_recv.at[q, (1 - d) // 2, i], to)

    def x_long(q, s, h, d, origin, to):
        piece = weights.at[q, half_at(h), (origin + 2 * side) % side, second_rows, :]
        i = long_index(s, h)
        return remote(piece, piece, xb_send.at[q, (1 - d) // 2, i], xb_recv.at[q, (1 - d) // 2, i], to)

    def long_send(q, s, h, d):
        y_long(q, s, h, d, y - d * (s - 1), y_to[d]).start()
        x_long(q, s, h, d, x - d * (s - 1), x_to[d]).start()

    def long_wait(q, s, h, d):
        y_long(q, s, h, d, y - d * s, y_to[d]).wait_recv()
        x_long(q, s, h, d, x - d * s, x_to[d]).wait_recv()

    def long_done(q, s, h, d):
        y_long(q, s, h, d, y - d * (s - 1), y_to[d]).wait_send()
        x_long(q, s, h, d, x - d * (s - 1), x_to[d]).wait_send()

    def across(q, i, origin, plane_rows):
        piece = weights.at[q, :, (origin + 2 * side) % side, plane_rows, :]
        return remote(piece, piece, z_send.at[q, i], z_recv.at[q, i], opposite)

    across_list = [(0, 0)]
    for s in range(1, reach):
        across_list += [(1 + 2 * (s - 1), s), (2 + 2 * (s - 1), -s)]
    across_list.append((side - 1, reach))

    def across_send(q, i):
        across(q, i, x - across_list[i][1], second_rows).start()

    prompt_size = n_tok * 2 * chips // PROMPTS
    base = (chip * 2 * n_tok) % prompt_size
    limit = lengths_ref[(chip * 2 * n_tok) // prompt_size]

    def normalise(start, count, step):
        def one(i, carry):
            at = pl.ds(pl.multiple_of(start + i * step, step), step)
            span = 512 if depth % 512 == 0 else 128
            squares = jnp.zeros((step, 128), jnp.float32)
            for lo in range(0, depth, 128):
                wide = rows[at, lo : lo + 128].astype(jnp.float32)
                squares += wide * wide
            mean = jnp.sum(squares, axis=1, keepdims=True) * (1.0 / depth)
            scale = lax.rsqrt(mean + EPS)
            for lo in range(0, depth, span):
                wide = rows[at, lo : lo + span].astype(jnp.float32)
                rows[at, lo : lo + span] = (
                    wide * scale * gain_ref[:, lo : lo + span].astype(jnp.float32)
                ).astype(jnp.bfloat16)
            return carry

        lax.fori_loop(0, count, one, 0)

    def tables():
        count = 32
        lane = lax.broadcasted_iota(jnp.int32, (count, HEAD), 1)
        step = lax.broadcasted_iota(jnp.int32, (count, HEAD), 0)

        def one(i, carry):
            angle = (base + i * count + step).astype(jnp.float32) * freq_ref[...]
            at = pl.ds(i * (count // PAGE), count // PAGE)
            cosine[at] = jnp.cos(angle).reshape(count // PAGE, PAGE, HEAD)
            turn = jnp.sin(angle)
            turn = jnp.where(lane < HEAD // 2, -turn, turn)
            sine[at] = turn.reshape(count // PAGE, PAGE, HEAD)
            return carry

        lax.fori_loop(0, 2 * n_tok // count, one, 0)

    pages = n_tok // PAGE

    def slot_table(owner, entry):
        lane = lax.broadcasted_iota(jnp.int32, (8, 128), 1)
        row = lax.broadcasted_iota(jnp.int32, (8, 128), 0)
        found = jnp.zeros((8, 128), jnp.int32)
        for p in range(pages):
            told = jnp.where(row == 0, p, limit)
            found = jnp.where(lane == lax.rem(entry(p), SLOTS), told, found)
        slot_vec[owner] = found

    def slot_copy():
        return pltpu.make_async_copy(
            slot_vec, slot_smem, local_sem.at[token_parts + CHUNKS + 3]
        )

    deep = side * block

    def multiply(q, k):
        w = weights[q, k].reshape(deep, width)
        step = 256 if (2 * n_tok) % 256 == 0 else 2 * n_tok
        at_k = pl.ds(pl.multiple_of(k * deep, 128), deep)

        def one(i, carry):
            at = pl.ds(pl.multiple_of(i * step, step), step)
            got = jnp.dot(rows[at, at_k], w, preferred_element_type=jnp.float32)
            got = got.reshape(step // PAGE, PAGE, width)
            at = pl.ds(i * (step // PAGE), step // PAGE)
            total[at] = jnp.where(k == 0, 0.0, total[at]) + got
            return carry

        lax.fori_loop(0, 2 * n_tok // step, one, 0)

    def page_rows(owner, slot, is_key):
        page = owner * pages + slot_smem[owner, 0, slot]
        end = slot_smem[owner, 1, slot]
        value = total[page]
        if is_key:
            cosines, sines = cosine[page], sine[page]
            turned = []
            for head in range(width // HEAD):
                a = value[:, head * HEAD : (head + 1) * HEAD]
                turned.append(a * cosines + pltpu.roll(a, HEAD // 2, 1) * sines)
            value = jnp.concatenate(turned, axis=1)
        position = base + page * PAGE + lax.broadcasted_iota(jnp.int32, value.shape, 0)
        return jnp.where(position < end, value, 0.0).astype(jnp.bfloat16)

    def out_columns(q, cc):
        return pl.ds(pl.multiple_of(cc * half_cols + (q % 2) * width, 128), width)

    def pages_out(q, is_key):
        kv = q // 2
        mine = out_columns(q, core)

        def one(j, carry):
            parcel[q, j] = page_rows(1, 3 * CAP + j, is_key)
            parcel[q, CAP + j] = page_rows(0, 4 * CAP + j, is_key)
            parcel[q, 2 * CAP + j] = page_rows(1, 4 * CAP + j, is_key)
            parcel[q, 3 * CAP + j] = page_rows(1, j, is_key)
            parcel[q, 4 * CAP + j] = page_rows(0, CAP + j, is_key)
            parcel[q, 5 * CAP + j] = page_rows(0, j, is_key)
            far = 1 - core
            parcel[q, 6 * CAP + j] = page_rows(1, (1 + far) * CAP + j, is_key)
            parcel[q, 7 * CAP + j] = page_rows(0, (2 + far) * CAP + j, is_key)
            near = (1 + core) * CAP + j
            out[kv, near, :, mine] = page_rows(1, near, is_key)
            near = (2 + core) * CAP + j
            out[kv, near, :, mine] = page_rows(0, near, is_key)
            return carry

        lax.fori_loop(0, CAP, one, 0)

    parcels = (
        (0, 2 * CAP, 3 * CAP, 1, 0),
        (2 * CAP, CAP, 4 * CAP, 1, 1),
        (3 * CAP, 2 * CAP, 0, -1, 1),
        (5 * CAP, CAP, 0, -1, 0),
    )

    def page_send_of(q, i):
        at, count, slot, where, cc = parcels[i]
        chip_to = next_chip if where == 1 else prev_chip
        return remote(
            parcel.at[q, pl.ds(at, count)],
            out.at[q // 2, pl.ds(slot, count), :, out_columns(q, core)],
            page_send.at[q, i],
            page_recv.at[q, (1 - where) // 2, core],
            (group, chip_to * 2 + cc),
        )

    def page_swap(q):
        slot = pl.multiple_of((2 - core) * CAP, CAP)
        return remote(
            parcel.at[q, pl.ds(6 * CAP, 2 * CAP)],
            out.at[q // 2, pl.ds(slot, 2 * CAP), :, out_columns(q, core)],
            page_send.at[q, 4],
            page_recv.at[q, 2, 0],
            partner,
        )

    def pages_send(q):
        for i in range(len(parcels)):
            page_send_of(q, i).start()
        page_swap(q).start()

    def pages_arrive(q, cc):
        for i, (at, count, slot, where, target) in enumerate(parcels):
            if target != cc:
                continue
            for sender in range(2):
                there = out.at[q // 2, pl.ds(slot, count), :, out_columns(q, sender)]
                remote(
                    there, there, page_send.at[q, i], page_recv.at[q, (1 - where) // 2, sender], partner
                ).wait_recv()
        there = out.at[q // 2, pl.ds((1 + cc) * CAP, 2 * CAP), :, out_columns(q, 1 - cc)]
        remote(there, there, page_send.at[q, 4], page_recv.at[q, 2, 0], partner).wait_recv()

    step = 32
    per_part = part // step

    block_ready(0)
    short_send(0, 1)
    block_ready(1)
    short_send(1, 1)
    jobs = [
        lambda: slot_table(core, lambda p: table_ref[0, p]),
        tables,
    ]
    for i in range(token_parts):

        def job(i=i):
            token_local(i).wait()
            normalise(core * n_tok + i * part, per_part, step)

        jobs.append(job)
    share = -(-len(jobs) // reach)
    for s in range(1, reach + 1):
        for job in jobs[(s - 1) * share : s * share]:
            job()
        for g in range(2):
            short_wait(g, s)
            if s < reach:
                short_send(g, s + 1)

    def advance(q, s, h):
        for d in (1, -1):
            if h in long_halves(s, d):
                if s > 1:
                    long_wait(q, s - 1, h, d)
                long_send(q, s, h, d)
            elif s > 1:
                long_wait(q, s - 1, h, d)
        if h == 1 and s > 1:
            across_send(q, 1 + 2 * (s - 2))
            across_send(q, 2 + 2 * (s - 2))

    def finish(q):
        for d in (1, -1):
            for h in long_halves(reach, d):
                long_wait(q, reach, h, d)
        across_send(q, side - 1)
        for i, (_, distance) in enumerate(across_list):
            across(q, i, x - distance, other_rows).wait_recv()

    def gather(q, work):
        across_send(q, 0)
        at = 0
        for s in range(1, reach + 1):
            for h in range(2):
                advance(q, s, h)
                if at < len(work):
                    work[at]()
                at += 1
        for left in work[at:]:
            left()
        finish(q)

    work = []
    for i in range(token_parts):

        def job(i=i):
            token_arrival(i).wait_recv()
            normalise((1 - core) * n_tok + i * part, per_part, step)

        work.append(job)

    def other_table():
        give_table().wait_recv()
        copy = pltpu.make_async_copy(
            table_vec, table_smem, local_sem.at[token_parts + CHUNKS + 2]
        )
        copy.start()
        copy.wait()
        slot_table(1 - core, lambda p: table_smem[0, p])
        copy = slot_copy()
        copy.start()
        copy.wait()

    work.append(other_table)
    gather(0, work)

    def multiply_some(q, some):
        def one(k, carry):
            multiply(q, k)
            return carry

        lax.fori_loop(some[0], some[1], one, 0)

    def hand_over(q, is_key):
        pages_out(q, is_key)
        pages_send(q)

    slots = 4
    for q in range(1, CHUNKS):
        work = []
        for i in range(slots):
            some = (i * side // slots, (i + 1) * side // slots)
            work.append(functools.partial(multiply_some, q - 1, some))
        work.append(functools.partial(hand_over, q - 1, q - 1 < CHUNKS // 2))
        gather(q, work)

    last = CHUNKS - 1
    multiply_some(last, (0, side))
    hand_over(last, last < CHUNKS // 2)

    for cc in range(2):

        @pl.when(core == cc)
        def _(cc=cc):
            for q in range(CHUNKS):
                if cc == 0:
                    give_first(q).wait_send()
                else:
                    give_second(q).wait_send()

    give_table().wait_send()
    for i in range(token_parts):
        token_swap(i).wait_send()
    for s in range(1, reach + 1):
        for g in range(2):
            short_done(g, s)

    def chunk_done(q, carry):
        for s in range(1, reach + 1):
            for d in (1, -1):
                for h in long_halves(s, d):
                    long_done(q, s, h, d)
        for i, (_, distance) in enumerate(across_list):
            across(q, i, x - distance, second_rows).wait_send()
        for i in range(len(parcels)):
            page_send_of(q, i).wait_send()
        page_swap(q).wait_send()
        return carry

    lax.fori_loop(0, CHUNKS, chunk_done, 0)
    for cc in range(2):

        @pl.when(core == cc)
        def _(cc=cc):
            def arrive(q, carry):
                pages_arrive(q, cc)
                return carry

            lax.fori_loop(0, CHUNKS, arrive, 0)


def on_device(tokens, norm_gain, w_key, w_value, lengths, page_table):
    n_seq = lax.axis_size("seq")
    side = math.isqrt(n_seq // 2)
    n_tok, depth = tokens.shape
    share, features = w_key.shape
    width = features // CHUNKS
    block = 2 * share
    pages = n_tok // PAGE
    assert 2 * side * side == n_seq and side % 2 == 0
    assert block == FIRST + 2 * SECOND and share == FIRST
    assert block * side * side == depth and width % HEAD == 0
    half = HEAD // 2
    freq = np.float32(ROPE_THETA) ** (-(np.arange(half, dtype=np.float32) * 2.0 / HEAD))
    freq = np.concatenate([freq, freq]).astype(np.float32)[None, :]
    reach = side // 2
    dma = pltpu.SemaphoreType.DMA
    vmem = pl.BlockSpec(memory_space=pltpu.VMEM)
    smem = pl.BlockSpec(memory_space=pltpu.SMEM)
    hbm = pl.BlockSpec(memory_space=pltpu.HBM)
    table = page_table.reshape(1, pages)
    long_sems = dma((CHUNKS, 2, 2 * reach - 1))
    return pl.pallas_call(
        functools.partial(kernel, side),
        out_shape=jax.ShapeDtypeStruct((2, SLOTS, PAGE, features), jnp.bfloat16),
        in_specs=[hbm, vmem, vmem, hbm, hbm, smem, smem, hbm],
        out_specs=vmem,
        scratch_shapes=[
            pltpu.VMEM((2 * n_tok, depth), jnp.bfloat16),
            pltpu.VMEM((CHUNKS, side, side, block, width), jnp.bfloat16),
            pltpu.VMEM((2, share, features // 2), jnp.bfloat16),
            pltpu.VMEM((2 * pages, PAGE, width), jnp.float32),
            pltpu.VMEM((2 * pages, PAGE, HEAD), jnp.float32),
            pltpu.VMEM((2 * pages, PAGE, HEAD), jnp.float32),
            pltpu.VMEM((CHUNKS, 8 * CAP, PAGE, width), jnp.bfloat16),
            pltpu.VMEM((1, pages), jnp.int32),
            pltpu.SMEM((1, pages), jnp.int32),
            pltpu.VMEM((2, 8, 128), jnp.int32),
            pltpu.SMEM((2, 8, 128), jnp.int32),
            dma((12,)),
            dma((9,)),
            dma((9,)),
            dma((2, 2, reach)),
            dma((2, 2, reach)),
            dma((2, 2, reach)),
            dma((2, 2, reach)),
            long_sems,
            long_sems,
            long_sems,
            long_sems,
            dma((CHUNKS, side)),
            dma((CHUNKS, side)),
            dma((CHUNKS, 5)),
            dma((CHUNKS, 3, 2)),
        ],
        compiler_params=pltpu.CompilerParams(
            collective_id=0,
            has_side_effects=True,
            vmem_limit_bytes=56 * 1024 * 1024,
        ),
    )(tokens, norm_gain[None, :], jnp.asarray(freq), w_key, w_value, lengths, table, table)


def solution(mesh):
    placed = (
        P(("group", "seq"), None),
        P(),
        P("seq", None),
        P("seq", None),
        P("group"),
        P(("group", "seq")),
    )
    return jax.shard_map(
        on_device,
        mesh=mesh,
        in_specs=placed,
        out_specs=P(None, ("group", "seq"), None, None),
        check_vma=False,
    )
```

```python
import functools
import math

import jax
import jax.numpy as jnp
import numpy as np
from jax import lax
from jax.experimental import pallas as pl
from jax.experimental.pallas import tpu as pltpu
from jax.sharding import PartitionSpec as P

HEAD = 128
PAGE = 16
REACH = 2
CAP = 8
SLOTS = 40
PROMPTS = 2

ROPE_THETA = 500000.0
EPS = 1e-05

MESH = pl.DeviceIdType.MESH
CHUNKS = 4
FIRST = 32
SECOND = 16


def kernel(
    side,
    tokens_hbm,
    gain_ref,
    freq_ref,
    wk_hbm,
    wv_hbm,
    lengths_ref,
    table_ref,
    table_hbm,
    out,
    rows,
    weights,
    stage,
    total,
    cosine,
    sine,
    parcel,
    table_vec,
    table_smem,
    slot_vec,
    slot_smem,
    local_sem,
    swap_send,
    swap_recv,
    xd_send,
    xd_recv,
    yd_send,
    yd_recv,
    xs_send,
    xs_recv,
    ys_send,
    ys_recv,
    xb_send,
    xb_recv,
    yb_send,
    yb_recv,
    z_send,
    z_recv,
    page_send,
    page_recv,
):
    n_tok, depth = tokens_hbm.shape
    width = weights.shape[4]
    half_cols = width * (CHUNKS // 2)
    reach = side // 2
    half = side // 2
    block = weights.shape[3]

    group = lax.axis_index("group")
    me = lax.axis_index("seq")
    core = me % 2
    chip = me // 2
    x = chip % side
    y = chip // side
    chips = side * side
    parity = group % 2

    def device(yy, xx, cc):
        index = (((yy + side) % side) * side + (xx + side) % side) * 2 + cc
        return (group, index)

    partner = (group, chip * 2 + 1 - core)
    opposite = (group + 1 - 2 * parity, me)
    next_chip = (chip + 1) % chips
    prev_chip = (chip + chips - 1) % chips
    x_to = {1: device(y, x + 1, core), -1: device(y, x - 1, core)}
    y_to = {1: device(y + 1, x, core), -1: device(y - 1, x, core)}

    first_rows = pl.ds(0, FIRST)
    second_rows = pl.ds(pl.multiple_of(FIRST + SECOND * parity, SECOND), SECOND)
    other_rows = pl.ds(pl.multiple_of(FIRST + SECOND * (1 - parity), SECOND), SECOND)
    shard_second = pl.ds(pl.multiple_of(SECOND * parity, SECOND), SECOND)

    sent = []

    def remote(src, dst, send_sem, recv_sem, to):
        return pltpu.make_async_remote_copy(
            src_ref=src,
            dst_ref=dst,
            send_sem=send_sem,
            recv_sem=recv_sem,
            device_id=to,
            device_id_type=MESH,
        )

    token_parts = 4
    part = n_tok // token_parts

    def token_local(i):
        return pltpu.make_async_copy(
            tokens_hbm.at[pl.ds(i * part, part)],
            rows.at[pl.ds(pl.multiple_of(core * n_tok + i * part, part), part)],
            local_sem.at[i],
        )

    def token_swap(i):
        return remote(
            tokens_hbm.at[pl.ds(i * part, part)],
            rows.at[pl.ds(pl.multiple_of(core * n_tok + i * part, part), part)],
            swap_send.at[i],
            swap_recv.at[i],
            partner,
        )

    def token_arrival(i):
        there = rows.at[pl.ds(pl.multiple_of((1 - core) * n_tok + i * part, part), part)]
        return remote(there, there, swap_send.at[i], swap_recv.at[i], partner)

    def columns_of(q, cc):
        return pl.ds(pl.multiple_of(cc * half_cols + (q % 2) * width, 128), width)

    def shard(q):
        return wk_hbm if q < CHUNKS // 2 else wv_hbm

    def own_first(q):
        return pltpu.make_async_copy(
            shard(q).at[:, columns_of(q, core)],
            weights.at[q, y, x, first_rows, :],
            local_sem.at[token_parts + q],
        )

    def own_second(q):
        return pltpu.make_async_copy(
            shard(q).at[shard_second, columns_of(q, core)],
            weights.at[q, y, x, second_rows, :],
            local_sem.at[token_parts + q],
        )

    def staged(kv):
        source = (wk_hbm, wv_hbm)[kv]
        return pltpu.make_async_copy(
            source.at[:, pl.ds(pl.multiple_of((1 - core) * half_cols, 128), half_cols)],
            stage.at[kv],
            local_sem.at[token_parts + CHUNKS + kv],
        )

    def give_first(q):
        return remote(
            stage.at[q // 2, :, pl.ds((q % 2) * width, width)],
            weights.at[q, y, x, first_rows, :],
            swap_send.at[token_parts + q],
            swap_recv.at[token_parts + q],
            partner,
        )

    def give_second(q):
        return remote(
            stage.at[q // 2, shard_second, pl.ds((q % 2) * width, width)],
            weights.at[q, y, x, second_rows, :],
            swap_send.at[token_parts + q],
            swap_recv.at[token_parts + q],
            partner,
        )

    def give_table():
        i = token_parts + CHUNKS
        return remote(
            table_hbm, table_vec, swap_send.at[i], swap_recv.at[i], partner
        )

    for kv in range(2):
        staged(kv).start()

    @pl.when(core == 0)
    def _():
        for q in range(CHUNKS):
            own_first(q).start()

    @pl.when(core == 1)
    def _():
        for q in range(CHUNKS):
            own_second(q).start()

    for i in range(token_parts):
        token_local(i).start()

    barrier = pltpu.get_barrier_semaphore()
    friends = [partner, opposite]
    for k in range(1, side):
        friends += [device(y, x + k, core), device(y + k, x, core)]
    for other in (next_chip, prev_chip):
        for cc in range(2):
            friends.append((group, other * 2 + cc))
    for friend in friends:
        pl.semaphore_signal(barrier, inc=1, device_id=friend, device_id_type=MESH)
    pl.semaphore_wait(barrier, len(friends))

    for kv in range(2):
        staged(kv).wait()

    @pl.when(core == 0)
    def _():
        for q in range(CHUNKS):
            give_first(q).start()

    @pl.when(core == 1)
    def _():
        for q in range(CHUNKS):
            give_second(q).start()

    give_table().start()
    for i in range(token_parts):
        token_swap(i).start()

    def x_direct(k, origin):
        piece = weights.at[0, y, (origin + side) % side, first_rows, :]
        return remote(piece, piece, xd_send.at[k - 1], xd_recv.at[k - 1], device(y, x + k, core))

    def y_direct(k, origin):
        piece = weights.at[0, (origin + side) % side, x, second_rows, :]
        return remote(piece, piece, yd_send.at[k - 1], yd_recv.at[k - 1], device(y + k, x, core))

    near_first = sorted(range(1, side), key=lambda k: min(k, side - k))

    def direct_wait():
        for k in near_first:
            x_direct(k, x - k).wait_recv()
            y_direct(k, y - k).wait_recv()

    later = pl.ds(1, CHUNKS - 1)

    def x_short(s, d, origin, to):
        piece = weights.at[later, y, (origin + 2 * side) % side, first_rows, :]
        i = (1 - d) // 2
        return remote(piece, piece, xs_send.at[i, s - 1], xs_recv.at[i, s - 1], to)

    def y_short(s, d, origin, to):
        piece = weights.at[later, (origin + 2 * side) % side, x, second_rows, :]
        i = (1 - d) // 2
        return remote(piece, piece, ys_send.at[i, s - 1], ys_recv.at[i, s - 1], to)

    def short_ways(s):
        return (1, -1) if s < reach else (-1,)

    def short_send(s):
        for d in short_ways(s):
            x_short(s, d, x - d * (s - 1), x_to[d]).start()
            y_short(s, d, y - d * (s - 1), y_to[d]).start()

    def short_wait(s):
        for d in short_ways(s):
            x_short(s, d, x - d * s, x_to[d]).wait_recv()
            y_short(s, d, y - d * s, y_to[d]).wait_recv()

    def short_done(s):
        for d in short_ways(s):
            x_short(s, d, x - d * (s - 1), x_to[d]).wait_send()
            y_short(s, d, y - d * (s - 1), y_to[d]).wait_send()

    def x_begin():
        for k in near_first:
            x_direct(k, x).start()
        for d in short_ways(1):
            x_short(1, d, x, x_to[d]).start()

    def y_begin():
        for k in near_first:
            y_direct(k, y).start()
        for d in short_ways(1):
            y_short(1, d, y, y_to[d]).start()

    def begin():
        @pl.when(core == 0)
        def _():
            for q in range(CHUNKS):
                own_first(q).wait()
            x_begin()
            for q in range(CHUNKS):
                give_second(q).wait_recv()
            y_begin()

        @pl.when(core == 1)
        def _():
            for q in range(CHUNKS):
                own_second(q).wait()
            y_begin()
            for q in range(CHUNKS):
                give_first(q).wait_recv()
            x_begin()

    def half_at(h):
        return pl.ds(h * half, half)

    def long_halves(s, d):
        if s < reach:
            return (0, 1)
        return (0,) if d == 1 else (1,)

    def long_index(s, h):
        return 2 * (s - 1) + (h if s < reach else 0)

    def y_long(q, s, h, d, origin, to):
        piece = weights.at[q, (origin + 2 * side) % side, half_at(h), first_rows, :]
        i = long_index(s, h)
        return remote(piece, piece, yb_send.at[q, (1 - d) // 2, i], yb_recv.at[q, (1 - d) // 2, i], to)

    def x_long(q, s, h, d, origin, to):
        piece = weights.at[q, half_at(h), (origin + 2 * side) % side, second_rows, :]
        i = long_index(s, h)
        return remote(piece, piece, xb_send.at[q, (1 - d) // 2, i], xb_recv.at[q, (1 - d) // 2, i], to)

    def long_send(q, s, h, d):
        y_long(q, s, h, d, y - d * (s - 1), y_to[d]).start()
        x_long(q, s, h, d, x - d * (s - 1), x_to[d]).start()

    def long_wait(q, s, h, d):
        y_long(q, s, h, d, y - d * s, y_to[d]).wait_recv()
        x_long(q, s, h, d, x - d * s, x_to[d]).wait_recv()

    def long_done(q, s, h, d):
        y_long(q, s, h, d, y - d * (s - 1), y_to[d]).wait_send()
        x_long(q, s, h, d, x - d * (s - 1), x_to[d]).wait_send()

    def across(q, i, origin, plane_rows):
        piece = weights.at[q, :, (origin + 2 * side) % side, plane_rows, :]
        return remote(piece, piece, z_send.at[q, i], z_recv.at[q, i], opposite)

    across_list = [(0, 0)]
    for s in range(1, reach):
        across_list += [(1 + 2 * (s - 1), s), (2 + 2 * (s - 1), -s)]
    across_list.append((side - 1, reach))

    def across_send(q, i):
        across(q, i, x - across_list[i][1], second_rows).start()

    prompt_size = n_tok * 2 * chips // PROMPTS
    base = (chip * 2 * n_tok) % prompt_size
    limit = lengths_ref[(chip * 2 * n_tok) // prompt_size]

    def normalise(start, count, step):
        def one(i, carry):
            at = pl.ds(pl.multiple_of(start + i * step, step), step)
            span = 512 if depth % 512 == 0 else 128
            squares = jnp.zeros((step, 128), jnp.float32)
            for lo in range(0, depth, 128):
                wide = rows[at, lo : lo + 128].astype(jnp.float32)
                squares += wide * wide
            mean = jnp.sum(squares, axis=1, keepdims=True) * (1.0 / depth)
            scale = lax.rsqrt(mean + EPS)
            for lo in range(0, depth, span):
                wide = rows[at, lo : lo + span].astype(jnp.float32)
                rows[at, lo : lo + span] = (
                    wide * scale * gain_ref[:, lo : lo + span].astype(jnp.float32)
                ).astype(jnp.bfloat16)
            return carry

        lax.fori_loop(0, count, one, 0)

    def tables():
        count = 32
        lane = lax.broadcasted_iota(jnp.int32, (count, HEAD), 1)
        step = lax.broadcasted_iota(jnp.int32, (count, HEAD), 0)

        def one(i, carry):
            angle = (base + i * count + step).astype(jnp.float32) * freq_ref[...]
            at = pl.ds(i * (count // PAGE), count // PAGE)
            cosine[at] = jnp.cos(angle).reshape(count // PAGE, PAGE, HEAD)
            turn = jnp.sin(angle)
            turn = jnp.where(lane < HEAD // 2, -turn, turn)
            sine[at] = turn.reshape(count // PAGE, PAGE, HEAD)
            return carry

        lax.fori_loop(0, 2 * n_tok // count, one, 0)

    pages = n_tok // PAGE

    def slot_table(owner, entry):
        lane = lax.broadcasted_iota(jnp.int32, (8, 128), 1)
        row = lax.broadcasted_iota(jnp.int32, (8, 128), 0)
        found = jnp.zeros((8, 128), jnp.int32)
        for p in range(pages):
            told = jnp.where(row == 0, p, limit)
            found = jnp.where(lane == lax.rem(entry(p), SLOTS), told, found)
        slot_vec[owner] = found

    def slot_copy():
        return pltpu.make_async_copy(
            slot_vec, slot_smem, local_sem.at[token_parts + CHUNKS + 3]
        )

    deep = side * block

    def multiply(q, k):
        w = weights[q, k].reshape(deep, width)
        step = 256 if (2 * n_tok) % 256 == 0 else 2 * n_tok
        at_k = pl.ds(pl.multiple_of(k * deep, 128), deep)

        def one(i, carry):
            at = pl.ds(pl.multiple_of(i * step, step), step)
            got = jnp.dot(rows[at, at_k], w, preferred_element_type=jnp.float32)
            got = got.reshape(step // PAGE, PAGE, width)
            at = pl.ds(i * (step // PAGE), step // PAGE)
            total[at] = jnp.where(k == 0, 0.0, total[at]) + got
            return carry

        lax.fori_loop(0, 2 * n_tok // step, one, 0)

    def page_rows(owner, slot, is_key):
        page = owner * pages + slot_smem[owner, 0, slot]
        end = slot_smem[owner, 1, slot]
        value = total[page]
        if is_key:
            cosines, sines = cosine[page], sine[page]
            turned = []
            for head in range(width // HEAD):
                a = value[:, head * HEAD : (head + 1) * HEAD]
                turned.append(a * cosines + pltpu.roll(a, HEAD // 2, 1) * sines)
            value = jnp.concatenate(turned, axis=1)
        position = base + page * PAGE + lax.broadcasted_iota(jnp.int32, value.shape, 0)
        return jnp.where(position < end, value, 0.0).astype(jnp.bfloat16)

    def out_columns(q, cc):
        return pl.ds(pl.multiple_of(cc * half_cols + (q % 2) * width, 128), width)

    def pages_out(q, is_key):
        kv = q // 2
        mine = out_columns(q, core)

        def one(j, carry):
            parcel[q, j] = page_rows(1, 3 * CAP + j, is_key)
            parcel[q, CAP + j] = page_rows(0, 4 * CAP + j, is_key)
            parcel[q, 2 * CAP + j] = page_rows(1, 4 * CAP + j, is_key)
            parcel[q, 3 * CAP + j] = page_rows(1, j, is_key)
            parcel[q, 4 * CAP + j] = page_rows(0, CAP + j, is_key)
            parcel[q, 5 * CAP + j] = page_rows(0, j, is_key)
            far = 1 - core
            parcel[q, 6 * CAP + j] = page_rows(1, (1 + far) * CAP + j, is_key)
            parcel[q, 7 * CAP + j] = page_rows(0, (2 + far) * CAP + j, is_key)
            near = (1 + core) * CAP + j
            out[kv, near, :, mine] = page_rows(1, near, is_key)
            near = (2 + core) * CAP + j
            out[kv, near, :, mine] = page_rows(0, near, is_key)
            return carry

        lax.fori_loop(0, CAP, one, 0)

    parcels = (
        (0, 2 * CAP, 3 * CAP, 1, 0),
        (2 * CAP, CAP, 4 * CAP, 1, 1),
        (3 * CAP, 2 * CAP, 0, -1, 1),
        (5 * CAP, CAP, 0, -1, 0),
    )

    def page_send_of(q, i):
        at, count, slot, where, cc = parcels[i]
        chip_to = next_chip if where == 1 else prev_chip
        return remote(
            parcel.at[q, pl.ds(at, count)],
            out.at[q // 2, pl.ds(slot, count), :, out_columns(q, core)],
            page_send.at[q, i],
            page_recv.at[q, (1 - where) // 2, core],
            (group, chip_to * 2 + cc),
        )

    def page_swap(q):
        slot = pl.multiple_of((2 - core) * CAP, CAP)
        return remote(
            parcel.at[q, pl.ds(6 * CAP, 2 * CAP)],
            out.at[q // 2, pl.ds(slot, 2 * CAP), :, out_columns(q, core)],
            page_send.at[q, 4],
            page_recv.at[q, 2, 0],
            partner,
        )

    def pages_send(q):
        for i in range(len(parcels)):
            page_send_of(q, i).start()
        page_swap(q).start()

    def pages_arrive(q, cc):
        for i, (at, count, slot, where, target) in enumerate(parcels):
            if target != cc:
                continue
            for sender in range(2):
                there = out.at[q // 2, pl.ds(slot, count), :, out_columns(q, sender)]
                remote(
                    there, there, page_send.at[q, i], page_recv.at[q, (1 - where) // 2, sender], partner
                ).wait_recv()
        there = out.at[q // 2, pl.ds((1 + cc) * CAP, 2 * CAP), :, out_columns(q, 1 - cc)]
        remote(there, there, page_send.at[q, 4], page_recv.at[q, 2, 0], partner).wait_recv()

    step = 32
    per_part = part // step

    def own_rows(i):
        token_local(i).wait()
        normalise(core * n_tok + i * part, per_part, step)

    def other_rows_in(i):
        token_arrival(i).wait_recv()
        normalise((1 - core) * n_tok + i * part, per_part, step)

    def slot_tables():
        give_table().wait_recv()
        copy = pltpu.make_async_copy(
            table_vec, table_smem, local_sem.at[token_parts + CHUNKS + 2]
        )
        copy.start()
        slot_table(core, lambda p: table_ref[0, p])
        copy.wait()
        slot_table(1 - core, lambda p: table_smem[0, p])
        slot_copy().start()

    def multiply_some(q, some):
        def one(k, carry):
            multiply(q, k)
            return carry

        lax.fori_loop(some[0], some[1], one, 0)

    def hand_over(q, is_key):
        pages_out(q, is_key)
        pages_send(q)

    lag = 2

    def advance(q, s, h):
        for d in (1, -1):
            if s > 1:
                long_wait(q, s - 1, h, d)
            if h in long_halves(s, d):
                long_send(q, s, h, d)
        if s == 1 and h == 1:
            across_send(q, 0)
        if h == 1 and s > 1:
            across_send(q, 1 + 2 * (s - 2))
            across_send(q, 2 + 2 * (s - 2))

    def finish(q):
        for d in (1, -1):
            for h in long_halves(reach, d):
                long_wait(q, reach, h, d)
        across_send(q, side - 1)

    def across_wait(q):
        for i, (_, distance) in enumerate(across_list):
            across(q, i, x - distance, other_rows).wait_recv()

    def pump(t, h):
        for q in range(CHUNKS):
            s = t - lag * q + 1
            if 1 <= s <= reach:
                advance(q, s, h)
            elif s == reach + 1 and h == 0:
                finish(q)

    points = {}

    def at(t, h, job):
        points.setdefault((t, h), []).append(job)

    for i in range(token_parts):
        at(i // 2, i % 2, functools.partial(own_rows, i))
        at(2 + i // 2, i % 2, functools.partial(other_rows_in, i))
    at(2, 1, slot_tables)
    for q in range(CHUNKS):
        t = lag * q + reach
        at(t, 1, functools.partial(across_wait, q))
        at(t, 1, functools.partial(multiply_some, q, (0, side // 2)))
        at(t + 1, 0, functools.partial(multiply_some, q, (side // 2, side)))
        if q == 0:
            at(t + 1, 0, lambda: slot_copy().wait())
        at(t + 1, 1, functools.partial(hand_over, q, q < CHUNKS // 2))

    begin()
    tables()
    short_wait(1)
    if reach > 1:
        short_send(2)
    direct_wait()
    for t in range(lag * (CHUNKS - 1) + reach + 2):
        for h in range(2):
            pump(t, h)
            s = 2 * t + h + 2
            if t < 2 and s <= reach:
                short_wait(s)
                if s < reach:
                    short_send(s + 1)
            for job in points.pop((t, h), ()):
                job()
    assert not points

    for cc in range(2):

        @pl.when(core == cc)
        def _(cc=cc):
            for q in range(CHUNKS):
                if cc == 0:
                    give_first(q).wait_send()
                else:
                    give_second(q).wait_send()

    give_table().wait_send()
    for i in range(token_parts):
        token_swap(i).wait_send()
    for s in range(1, reach + 1):
        short_done(s)
    for k in near_first:
        x_direct(k, x).wait_send()
        y_direct(k, y).wait_send()

    def chunk_done(q, carry):
        for s in range(1, reach + 1):
            for d in (1, -1):
                for h in long_halves(s, d):
                    long_done(q, s, h, d)
        for i, (_, distance) in enumerate(across_list):
            across(q, i, x - distance, second_rows).wait_send()
        for i in range(len(parcels)):
            page_send_of(q, i).wait_send()
        page_swap(q).wait_send()
        return carry

    lax.fori_loop(0, CHUNKS, chunk_done, 0)
    for cc in range(2):

        @pl.when(core == cc)
        def _(cc=cc):
            def arrive(q, carry):
                pages_arrive(q, cc)
                return carry

            lax.fori_loop(0, CHUNKS, arrive, 0)


def on_device(tokens, norm_gain, w_key, w_value, lengths, page_table):
    n_seq = lax.axis_size("seq")
    side = math.isqrt(n_seq // 2)
    n_tok, depth = tokens.shape
    share, features = w_key.shape
    width = features // CHUNKS
    block = 2 * share
    pages = n_tok // PAGE
    assert 2 * side * side == n_seq and side % 2 == 0
    assert block == FIRST + 2 * SECOND and share == FIRST
    assert block * side * side == depth and width % HEAD == 0
    half = HEAD // 2
    freq = np.float32(ROPE_THETA) ** (-(np.arange(half, dtype=np.float32) * 2.0 / HEAD))
    freq = np.concatenate([freq, freq]).astype(np.float32)[None, :]
    reach = side // 2
    dma = pltpu.SemaphoreType.DMA
    vmem = pl.BlockSpec(memory_space=pltpu.VMEM)
    smem = pl.BlockSpec(memory_space=pltpu.SMEM)
    hbm = pl.BlockSpec(memory_space=pltpu.HBM)
    table = page_table.reshape(1, pages)
    long_sems = dma((CHUNKS, 2, 2 * reach - 1))
    return pl.pallas_call(
        functools.partial(kernel, side),
        out_shape=jax.ShapeDtypeStruct((2, SLOTS, PAGE, features), jnp.bfloat16),
        in_specs=[hbm, vmem, vmem, hbm, hbm, smem, smem, hbm],
        out_specs=vmem,
        scratch_shapes=[
            pltpu.VMEM((2 * n_tok, depth), jnp.bfloat16),
            pltpu.VMEM((CHUNKS, side, side, block, width), jnp.bfloat16),
            pltpu.VMEM((2, share, features // 2), jnp.bfloat16),
            pltpu.VMEM((2 * pages, PAGE, width), jnp.float32),
            pltpu.VMEM((2 * pages, PAGE, HEAD), jnp.float32),
            pltpu.VMEM((2 * pages, PAGE, HEAD), jnp.float32),
            pltpu.VMEM((CHUNKS, 8 * CAP, PAGE, width), jnp.bfloat16),
            pltpu.VMEM((1, pages), jnp.int32),
            pltpu.SMEM((1, pages), jnp.int32),
            pltpu.VMEM((2, 8, 128), jnp.int32),
            pltpu.SMEM((2, 8, 128), jnp.int32),
            dma((12,)),
            dma((9,)),
            dma((9,)),
            dma((side - 1,)),
            dma((side - 1,)),
            dma((side - 1,)),
            dma((side - 1,)),
            dma((2, reach)),
            dma((2, reach)),
            dma((2, reach)),
            dma((2, reach)),
            long_sems,
            long_sems,
            long_sems,
            long_sems,
            dma((CHUNKS, side)),
            dma((CHUNKS, side)),
            dma((CHUNKS, 5)),
            dma((CHUNKS, 3, 2)),
        ],
        compiler_params=pltpu.CompilerParams(
            collective_id=0,
            has_side_effects=True,
            vmem_limit_bytes=56 * 1024 * 1024,
        ),
    )(tokens, norm_gain[None, :], jnp.asarray(freq), w_key, w_value, lengths, table, table)


def solution(mesh):
    placed = (
        P(("group", "seq"), None),
        P(),
        P("seq", None),
        P("seq", None),
        P("group"),
        P(("group", "seq")),
    )
    return jax.shard_map(
        on_device,
        mesh=mesh,
        in_specs=placed,
        out_specs=P(None, ("group", "seq"), None, None),
        check_vma=False,
    )
```
